32 devices in a mesh: section: 4 (over x, core), row: 2 (over y), col: 4 (over z).
Axes of the slice: x: 2, y: 2, z: 4, core: 2. Of those that a mesh axis runs over, the one named last changes fastest.
Arguments:
- hidden: bfloat16 [4, 8, 4096], P(None, None, 'col'), may hold values from -6 to 6
- norm_gain: bfloat16 [4, 4096], P('section', 'col'), may hold values from 0.25 to 1.75
- w_qkv: bfloat16 [4, 4096, 6144], P('section', 'col', 'row'), may hold values from -0.09375 to 0.09375
- w_out: bfloat16 [4, 4096, 4096], P('section', 'row', 'col'), may hold values from -0.09375 to 0.09375
- cache_keys: bfloat16 [4, 4, 8, 128, 8, 128], P('section', None, 'col', None, 'row'), may hold values from -240 to 240, as said below
- cache_values: bfloat16 [4, 4, 8, 128, 8, 128], P('section', None, 'col', None, 'row'), may hold values from -6 to 6
- cache_lengths: int32 [4, 8], P(None, 'col'), may hold values from 1 to 127
Outputs:
- layer_outputs: bfloat16 [4, 4, 8, 4096], P('section', None, None, 'col')
The draws below stay inside these ranges and needn't reach their ends.
Inputs may be any that keep to these rules, and one draw needn't show every extreme that they name: `cache_keys`: cached keys are of order one except that some sequences may carry much larger keys at a few positions.
All inputs are finite; a program needn't handle non-finite values.
Results may differ from the reference program's by a relative error of at most 0.04.
Values may be sent and summed in bfloat16 or wider, within the bound.
A program may use at most 64 MiB of HBM per device.

```python
import jax
import jax.numpy as jnp
from jax import lax

D = 4096
HEADS = 32
KVH = 8
HD = 128
MICRO = 4
LEN = 128
LAYERS = 4
BATCH = 8


def draw_cache_keys(key, part):
    normal_draw = jnp.clip(jax.random.normal(key, (LAYERS, MICRO, BATCH, LEN, KVH, HD), jnp.float32), -6.0, 6.0)
    return normal_draw.astype(jnp.bfloat16)


def touch_ends(drawn, rng, low, top_value):
    extent = drawn.shape
    spot = [jax.random.randint(jax.random.fold_in(rng, axis), (), 0, extent[axis]) for axis in range(len(extent))]
    drawn = drawn.at[tuple(spot)].set(low)
    longest = extent.index(max(extent))
    spot[longest] = (spot[longest] + 1) % extent[longest]
    return drawn.at[tuple(spot)].set(top_value)


def steps_of(rng, extent, pieces, smallest, top_value):
    loudness, own = 1.0, jax.random.fold_in(rng, 6)
    for position, blocks in pieces:
        draws = jnp.exp(jax.random.uniform(jax.random.fold_in(own, position), (blocks,), jnp.float32, smallest / len(pieces), top_value / len(pieces)))
        loudness = loudness * jnp.repeat(draws, extent[position] // blocks).reshape([-1 if axis == position else 1 for axis in range(len(extent))])
    return loudness


def noise(stream_key, extent, width, limit, cuts=(), kind=jnp.bfloat16):
    array = jax.random.normal(stream_key, extent, jnp.float32) * width
    if len(cuts) > 0:
        array = steps_of(stream_key, extent, cuts, -0.22, 0.18) * array
    return jnp.clip(array, min=-limit, max=limit).astype(kind)


def setup_inputs(seed: int = 0) -> dict:
    seeds = jax.random.split(jax.random.key(seed), 8)
    hidden = noise(seeds[0], (MICRO, BATCH, D), 1.0, 6.0, ((2, 4),))
    norm_gain = jnp.clip(1.0 + 0.15 * jax.random.normal(seeds[1], (LAYERS, D), jnp.float32), 0.25, 1.75).astype(jnp.bfloat16)
    w_qkv = noise(seeds[2], (LAYERS, D, (HEADS + 2 * KVH) * HD), D ** -0.5, 0.09375, ((0, 4), (1, 4), (2, 2)))
    w_out = noise(seeds[3], (LAYERS, HEADS * HD, D), (HEADS * HD) ** -0.5, 0.09375, ((0, 4), (1, 2), (2, 4)))
    cache_keys = draw_cache_keys(jax.random.fold_in(seeds[7], 71), 0)
    cache_values = noise(seeds[5], (LAYERS, MICRO, BATCH, LEN, KVH, HD), 1.0, 6.0, ((0, 4), (2, 4), (4, 2)))
    cache_lengths = touch_ends(jax.random.randint(seeds[6], (MICRO, BATCH), 1, LEN), jax.random.fold_in(seeds[6], 1), 1, LEN - 1).astype(jnp.int32)
    return {"hidden": hidden, "norm_gain": norm_gain, "w_qkv": w_qkv, "w_out": w_out, "cache_keys": cache_keys, "cache_values": cache_values, "cache_lengths": cache_lengths}


def rotate(vectors, positions):
    half_dim = vectors.shape[-1] // 2
    inverse_freq = 500000.0 ** (-jnp.arange(half_dim, dtype=jnp.float32) * 2.0 / vectors.shape[-1])
    angles = positions * inverse_freq
    angles = jnp.concatenate([angles, angles], axis=-1)
    swapped = jnp.concatenate([-vectors[..., half_dim:], vectors[..., :half_dim]], axis=-1)
    return vectors * jnp.cos(angles) + swapped * jnp.sin(angles)

def attend(queries, new_key, new_value, key_block, value_block, length):
    score_scale = 1.0 / jnp.sqrt(jnp.float32(queries.shape[-1]))
    scores = jnp.einsum('bgrd,bjgd->bgrj', queries.astype(jnp.float32), key_block.astype(jnp.float32)) * score_scale
    own_score = jnp.einsum('bgrd,bgd->bgr', queries.astype(jnp.float32), new_key.astype(jnp.float32)) * score_scale
    visible = jnp.arange(key_block.shape[1])[None, :] < length[:, None]
    scores = jnp.where(visible[:, None, None, :], scores, -jnp.inf)
    row_max = jnp.maximum(lax.optimization_barrier(jnp.max(scores, axis=-1)), own_score)
    cache_exp = jnp.exp(scores - row_max[..., None])
    own_exp = jnp.exp(own_score - row_max)
    total = lax.optimization_barrier(jnp.sum(cache_exp, axis=-1)) + own_exp
    cache_weight = (cache_exp / total[..., None]).astype(jnp.bfloat16)
    own_weight = (own_exp / total).astype(jnp.bfloat16)
    result = jnp.einsum('bgrj,bjgd->bgrd', cache_weight.astype(jnp.float32), value_block.astype(jnp.float32))
    result = result + own_weight.astype(jnp.float32)[..., None] * new_value.astype(jnp.float32)[:, :, None, :]
    return result.astype(jnp.bfloat16)

def heads_part(projected, key_block, value_block, length):
    per_group = projected.shape[2] - 2
    positions = length.astype(jnp.float32)
    queries = rotate(projected[:, :, :per_group], positions[:, None, None, None]).astype(jnp.bfloat16)
    new_key = rotate(projected[:, :, per_group], positions[:, None, None]).astype(jnp.bfloat16)
    new_value = projected[:, :, per_group + 1].astype(jnp.bfloat16)
    attended = attend(queries, new_key, new_value, key_block, value_block, length)
    return attended.reshape(attended.shape[0], -1)

def decoder_layer(current, gain_row, proj_weight, out_weight, key_block, value_block, length):
    h_float = current.astype(jnp.float32)
    scaled = (h_float * gain_row.astype(jnp.float32)).astype(jnp.bfloat16)
    squares = lax.optimization_barrier(jnp.sum(h_float * h_float, axis=1))
    factor = lax.rsqrt(squares / D + 1e-05)
    projected = jnp.dot(scaled, proj_weight, preferred_element_type=jnp.float32) * factor[:, None]
    projected = projected.reshape(current.shape[0], KVH, HEADS // KVH + 2, HD)
    attended = heads_part(projected, key_block, value_block, length)
    mixed_rows = jnp.dot(attended, out_weight, preferred_element_type=jnp.float32)
    return (h_float + mixed_rows).astype(jnp.bfloat16)

def reference(hidden, norm_gain, w_qkv, w_out, cache_keys, cache_values, cache_lengths):
    current = hidden
    collected = []
    for layer_at in range(LAYERS):
        produced = []
        for micro_at in range(MICRO):
            produced.append(decoder_layer(current[micro_at], norm_gain[layer_at], w_qkv[layer_at], w_out[layer_at], cache_keys[layer_at, micro_at], cache_values[layer_at, micro_at], cache_lengths[micro_at]))
        current = jnp.stack(produced)
        collected.append(current)
    return jnp.stack(collected)
```

```python
import functools
import math

import jax
import jax.numpy as jnp
from jax import lax
from jax.experimental import pallas as pl
from jax.experimental.pallas import tpu as pltpu
from jax.sharding import PartitionSpec as P

D = 4096
HEADS = 32
KVH = 8
MESH = pl.DeviceIdType.MESH


def remainder(values, by):
    if by & (by - 1) == 0:
        return values & (by - 1)
    return lax.rem(values, jnp.full_like(values, by))


def kernel(
    dims,
    hidden,
    gain,
    wq_hbm,
    wo_hbm,
    keys_hbm,
    values_hbm,
    lengths,
    out,
    wq,
    wo,
    keys,
    values,
    state,
    part,
    part_in,
    square,
    square_in,
    q_rows,
    k_rows,
    v_rows,
    a_rows,
    attended,
    mixed,
    arrived,
    load_sem,
    rs_send,
    rs_recv,
    sq_send,
    sq_recv,
    at_send,
    at_recv,
    x_send,
    x_recv,
    y_send,
    y_recv,
):
    sections, row_count, cols = dims
    s = lax.axis_index("section")
    r = lax.axis_index("row")
    c = lax.axis_index("col")
    micro, batch, depth = hidden.shape
    rows = micro * batch
    own = rows // cols
    seq_part = batch // cols
    groups, chunk = wq.shape[0], wq.shape[2]
    head_dim = keys.shape[2]
    per = HEADS // KVH
    heads = groups * per
    spots = keys.shape[1]
    pieces, piece = mixed.shape[1], mixed.shape[3]

    def remote(src, dst, send_sem, recv_sem, device):
        return pltpu.make_async_remote_copy(
            src_ref=src,
            dst_ref=dst,
            send_sem=send_sem,
            recv_sem=recv_sem,
            device_id=device,
            device_id_type=MESH,
        )

    loads = [
        pltpu.make_async_copy(
            wq_hbm.at[:, pl.ds(g * chunk, chunk)], wq.at[g], load_sem.at[g]
        )
        for g in range(groups)
    ]
    load_keys = pltpu.make_async_copy(keys_hbm, keys, load_sem.at[groups])
    load_values = pltpu.make_async_copy(values_hbm, values, load_sem.at[groups + 1])
    load_wo = pltpu.make_async_copy(wo_hbm, wo, load_sem.at[groups + 2])
    for load in loads + [load_keys, load_values, load_wo]:
        load.start()

    barrier = pltpu.get_barrier_semaphore()
    greeted = 0
    for k in range(1, cols):
        pl.semaphore_signal(
            barrier, inc=1, device_id=(s, r, lax.rem(c + k, cols)), device_id_type=MESH
        )
        greeted += 1
    for k in range(1, row_count):
        pl.semaphore_signal(
            barrier, inc=1, device_id=(s, lax.rem(r + k, row_count), c), device_id_type=MESH
        )
        greeted += 1
    for step in (1, sections - 1):
        for other in range(row_count):
            pl.semaphore_signal(
                barrier,
                inc=1,
                device_id=(lax.rem(s + step, sections), other, c),
                device_id_type=MESH,
            )
            greeted += 1

    to_row = lax.broadcasted_iota(jnp.int32, (rows, rows), 0)
    from_row = lax.broadcasted_iota(jnp.int32, (rows, rows), 1)
    order = jnp.zeros((rows, rows), jnp.bool_)
    back = jnp.zeros((rows, rows), jnp.bool_)
    for at in range(cols):
        for m in range(micro):
            first, source = at * own + m * seq_part, m * batch + at * seq_part
            inside = (to_row >= first) & (to_row < first + seq_part)
            order = order | (inside & (to_row - from_row == first - source))
            inside = (from_row >= first) & (from_row < first + seq_part)
            back = back | (inside & (from_row - to_row == first - source))
    order = jnp.where(order, 1.0, 0.0).astype(jnp.bfloat16)
    back = jnp.where(back, 1.0, 0.0).astype(jnp.bfloat16)

    row_at = lax.broadcasted_iota(jnp.int32, (own, head_dim), 0)
    lane = lax.broadcasted_iota(jnp.int32, (own, head_dim), 1)
    position = jnp.zeros((own, head_dim), jnp.float32)
    length_of = []
    for m in range(micro):
        for b in range(seq_part):
            length_of.append(lengths[m, b])
            position = jnp.where(
                row_at == m * seq_part + b, length_of[-1].astype(jnp.float32), position
            )
    half = head_dim // 2
    half_lane = jnp.where(lane < half, lane, lane - half).astype(jnp.float32)
    angles = position * jnp.exp(half_lane * (-2.0 * math.log(500000.0) / head_dim))
    cosine = jnp.cos(angles)
    sine = jnp.sin(angles)
    sine = jnp.where(lane < half, -sine, sine)

    def rotate(vectors):
        return vectors * cosine + pltpu.roll(vectors, half, 1) * sine

    head_at = lax.broadcasted_iota(jnp.int32, (heads, spots), 0)
    spot_at = lax.broadcasted_iota(jnp.int32, (heads, spots), 1)
    head_group = jnp.zeros((heads, spots), jnp.int32)
    for g in range(1, groups):
        head_group = head_group + jnp.where(head_at >= g * per, 1, 0)
    same_group = remainder(spot_at, groups) == head_group

    pl.semaphore_wait(barrier, greeted)

    @pl.when(s == 0)
    def _():
        entry = hidden[...].astype(jnp.float32).reshape(rows, depth).astype(jnp.bfloat16)
        state[...] = jnp.dot(order, entry, preferred_element_type=jnp.float32)

    @pl.when(s > 0)
    def _():
        for n in range(pieces):
            for other in range(row_count):
                remote(
                    mixed.at[0, n],
                    arrived.at[other, n],
                    x_send.at[n, 0],
                    x_recv.at[n, other],
                    (s, r, c),
                ).wait_recv()
            total = arrived[0, n]
            for other in range(1, row_count):
                total = total + arrived[other, n]
            state[:, n * piece : (n + 1) * piece] = total.astype(jnp.bfloat16).astype(jnp.float32)

    current = state[...]
    squares = jnp.sum(current * current, axis=1, keepdims=True)
    square[...] = jnp.broadcast_to(squares, (rows, head_dim)).reshape(cols, own, head_dim)
    copies = []
    for k in range(1, cols):
        peer = lax.rem(c + k, cols)
        copies.append(
            remote(
                square.at[peer],
                square_in.at[k - 1],
                sq_send.at[k - 1],
                sq_recv.at[k - 1],
                (s, r, peer),
            )
        )
        copies[-1].start()
    square_copies = copies[:]
    scaled = (current * gain[...].astype(jnp.float32)).astype(jnp.bfloat16)
    part_copies = []
    for g in range(groups):
        loads[g].wait()
        product = jnp.dot(scaled, wq[g], preferred_element_type=jnp.float32)
        part[g] = product.reshape(cols, own, chunk)
        started = []
        for k in range(1, cols):
            peer = lax.rem(c + k, cols)
            started.append(
                remote(
                    part.at[g, peer],
                    part_in.at[g, k - 1],
                    rs_send.at[g, k - 1],
                    rs_recv.at[g, k - 1],
                    (s, r, peer),
                )
            )
            started[-1].start()
        part_copies.append(started)
        copies = copies + started

    for copy in square_copies:
        copy.wait_recv()
    total = square[c]
    for k in range(1, cols):
        total = total + square_in[k - 1]
    factor = lax.rsqrt(total / D + 1e-05)
    for g in range(groups):
        for copy in part_copies[g]:
            copy.wait_recv()
        total = part[g, c]
        for k in range(1, cols):
            total = total + part_in[g, k - 1]
        cut = [total[:, i * head_dim : (i + 1) * head_dim] * factor for i in range(per + 2)]
        new_key = rotate(cut[per]).astype(jnp.bfloat16).astype(jnp.float32)
        new_value = cut[per + 1].astype(jnp.bfloat16).astype(jnp.float32)
        for i in range(per):
            at = pl.ds((g * per + i) * own, own)
            q_rows[at, :] = rotate(cut[i])
            k_rows[at, :] = new_key
            v_rows[at, :] = new_value
    load_keys.wait()
    load_values.wait()
    scale = 1.0 / math.sqrt(head_dim)
    seqs = range(own)
    taken = [pl.ds(i, heads, stride=own) for i in seqs]
    queries = [q_rows[taken[i], :].astype(jnp.bfloat16) for i in seqs]
    scores = [
        lax.dot_general(
            queries[i], keys[i], (((1,), (1,)), ((), ())), preferred_element_type=jnp.float32
        )
        * scale
        for i in seqs
    ]
    own_scores = [
        jnp.sum(queries[i].astype(jnp.float32) * k_rows[taken[i], :], axis=1, keepdims=True) * scale
        for i in seqs
    ]
    weights, own_weights = [], []
    for i in seqs:
        visible = same_group & (spot_at < length_of[i] * groups)
        masked = jnp.where(visible, scores[i], -jnp.inf)
        row_max = jnp.maximum(jnp.max(masked, axis=1, keepdims=True), own_scores[i])
        cache_exp = jnp.exp(masked - row_max)
        own_exp = jnp.exp(own_scores[i] - row_max)
        total = jnp.sum(cache_exp, axis=1, keepdims=True) + own_exp
        weights.append((cache_exp / total).astype(jnp.bfloat16))
        own_weights.append((own_exp / total).astype(jnp.bfloat16).astype(jnp.float32))
    for i in seqs:
        result = jnp.dot(weights[i], values[i], preferred_element_type=jnp.float32)
        a_rows[taken[i], :] = result + own_weights[i] * v_rows[taken[i], :]
    for h in range(heads):
        attended[c, :, h * head_dim : (h + 1) * head_dim] = a_rows[
            h * own : (h + 1) * own, :
        ].astype(jnp.bfloat16)
    started = []
    for k in range(1, cols):
        peer = lax.rem(c + k, cols)
        started.append(
            remote(
                attended.at[c],
                attended.at[c],
                at_send.at[k - 1],
                at_recv.at[k - 1],
                (s, r, peer),
            )
        )
        started[-1].start()
    copies = copies + started
    load_wo.wait()
    for copy in started:
        copy.wait_recv()

    everyone = (
        attended[...].astype(jnp.float32).reshape(rows, heads * head_dim).astype(jnp.bfloat16)
    )

    def onward(n, other):
        return remote(
            mixed.at[r, n],
            arrived.at[r, n],
            x_send.at[n, other],
            x_recv.at[n, r],
            (lax.rem(s + 1, sections), other, c),
        )

    sideways = []
    for n in range(pieces):
        at = slice(n * piece, (n + 1) * piece)
        product = jnp.dot(everyone, wo[:, at], preferred_element_type=jnp.float32)
        mixed[r, n] = product + jnp.where(r == 0, state[:, at], 0.0)

        @pl.when(s < sections - 1)
        def _():
            for other in range(row_count):
                onward(n, other).start()

    for n in range(pieces):
        for k in range(1, row_count):
            peer = lax.rem(r + k, row_count)
            sideways.append(
                remote(
                    mixed.at[r, n],
                    mixed.at[r, n],
                    y_send.at[n, k - 1],
                    y_recv.at[n, k - 1],
                    (s, peer, c),
                )
            )
            sideways[-1].start()
    for copy in sideways:
        copy.wait_recv()
    for n in range(pieces):
        total = mixed[0, n]
        for other in range(1, row_count):
            total = total + mixed[other, n]
        final = jnp.dot(back, total.astype(jnp.bfloat16), preferred_element_type=jnp.float32)
        out[:, :, n * piece : (n + 1) * piece] = final.reshape(micro, batch, piece).astype(
            jnp.bfloat16
        )

    for copy in copies + sideways:
        copy.wait_send()

    @pl.when(s < sections - 1)
    def _():
        for n in range(pieces):
            for other in range(row_count):
                onward(n, other).wait_send()


def shards(hidden, norm_gain, w_qkv, w_out, cache_keys, cache_values, cache_lengths):
    sections, row_count, cols = (lax.axis_size(a) for a in ("section", "row", "col"))
    micro, batch, depth = hidden.shape
    rows = micro * batch
    own = rows // cols
    seqs, spots, groups, head_dim = own, cache_keys.shape[3], *cache_keys.shape[4:]
    per = HEADS // KVH
    heads = groups * per
    chunk = (per + 2) * head_dim
    piece = min(256, w_out.shape[2])
    pieces = w_out.shape[2] // piece
    keys = cache_keys.reshape(seqs, spots * groups, head_dim)
    values = cache_values.reshape(seqs, spots * groups, head_dim)
    vmem = pl.BlockSpec(memory_space=pltpu.VMEM)
    hbm = pl.BlockSpec(memory_space=pl.ANY)
    dma = pltpu.SemaphoreType.DMA
    f32, bf16 = jnp.float32, jnp.bfloat16
    return pl.pallas_call(
        functools.partial(kernel, (sections, row_count, cols)),
        out_shape=jax.ShapeDtypeStruct((micro, batch, depth), bf16),
        in_specs=[vmem, vmem, hbm, hbm, hbm, hbm, pl.BlockSpec(memory_space=pltpu.SMEM)],
        out_specs=vmem,
        scratch_shapes=[
            pltpu.VMEM((groups, depth, chunk), bf16),
            pltpu.VMEM(w_out.shape[1:], bf16),
            pltpu.VMEM(keys.shape, bf16),
            pltpu.VMEM(values.shape, bf16),
            pltpu.VMEM((rows, depth), f32),
            pltpu.VMEM((groups, cols, own, chunk), f32),
            pltpu.VMEM((groups, cols - 1, own, chunk), f32),
            pltpu.VMEM((cols, own, head_dim), f32),
            pltpu.VMEM((cols - 1, own, head_dim), f32),
            pltpu.VMEM((heads * own, head_dim), f32),
            pltpu.VMEM((heads * own, head_dim), f32),
            pltpu.VMEM((heads * own, head_dim), f32),
            pltpu.VMEM((heads * own, head_dim), f32),
            pltpu.VMEM((cols, own, heads * head_dim), bf16),
            pltpu.VMEM((row_count, pieces, rows, piece), f32),
            pltpu.VMEM((row_count, pieces, rows, piece), f32),
            dma((groups + 3,)),
            dma((groups, cols - 1)),
            dma((groups, cols - 1)),
            dma((cols - 1,)),
            dma((cols - 1,)),
            dma((cols - 1,)),
            dma((cols - 1,)),
            dma((pieces, row_count)),
            dma((pieces, row_count)),
            dma((pieces, row_count - 1)),
            dma((pieces, row_count - 1)),
        ],
        compiler_params=pltpu.CompilerParams(collective_id=0, has_side_effects=True),
    )(hidden, norm_gain, w_qkv[0], w_out[0], keys, values, cache_lengths)[None]


def solution(mesh):
    return jax.shard_map(
        shards,
        mesh=mesh,
        in_specs=(
            P(None, None, "col"),
            P("section", "col"),
            P("section", "col", "row"),
            P("section", "row", "col"),
            P("section", None, "col", None, "row", None),
            P("section", None, "col", None, "row", None),
            P(None, "col"),
        ),
        out_specs=P("section", None, None, "col"),
        check_vma=False,
    )
```

```python
import functools
import math

import jax
import jax.numpy as jnp
from jax import lax
from jax.experimental import pallas as pl
from jax.experimental.pallas import tpu as pltpu
from jax.sharding import PartitionSpec as P

D = 4096
HEADS = 32
KVH = 8
LOTS = 2
MESH = pl.DeviceIdType.MESH


def remainder(values, by):
    if by & (by - 1) == 0:
        return values & (by - 1)
    return lax.rem(values, jnp.full_like(values, by))


def kernel(
    dims,
    hidden,
    gain,
    wq_hbm,
    wo_hbm,
    keys_hbm,
    values_hbm,
    lengths,
    out,
    wq,
    wo,
    keys,
    values,
    state,
    part,
    part_in,
    square,
    square_in,
    q_rows,
    k_rows,
    v_rows,
    a_rows,
    attended,
    gathered,
    mixed,
    arrived,
    load_sem,
    rs_send,
    rs_recv,
    sq_send,
    sq_recv,
    at_send,
    at_recv,
    x_send,
    x_recv,
    y_send,
    y_recv,
):
    sections, row_count, cols = dims
    s = lax.axis_index("section")
    r = lax.axis_index("row")
    c = lax.axis_index("col")
    batch, depth = hidden.shape[1:]
    lots, rows = state.shape[:2]
    micro = rows // batch
    own = rows // cols
    seq_part = batch // cols
    groups, chunk = wq.shape[0], wq.shape[2]
    head_dim = keys.shape[2]
    per = HEADS // KVH
    heads = groups * per
    spots = keys.shape[1]
    pieces, piece = mixed.shape[2], mixed.shape[4]

    def remote(src, dst, send_sem, recv_sem, device):
        return pltpu.make_async_remote_copy(
            src_ref=src,
            dst_ref=dst,
            send_sem=send_sem,
            recv_sem=recv_sem,
            device_id=device,
            device_id_type=MESH,
        )

    loads = [
        pltpu.make_async_copy(
            wq_hbm.at[:, pl.ds(g * chunk, chunk)], wq.at[g], load_sem.at[g]
        )
        for g in range(groups)
    ]
    load_keys = pltpu.make_async_copy(keys_hbm, keys, load_sem.at[groups])
    load_values = pltpu.make_async_copy(values_hbm, values, load_sem.at[groups + 1])
    load_wo = pltpu.make_async_copy(wo_hbm, wo, load_sem.at[groups + 2])
    for load in loads + [load_keys, load_values, load_wo]:
        load.start()

    barrier = pltpu.get_barrier_semaphore()
    greeted = 0
    for k in range(1, cols):
        pl.semaphore_signal(
            barrier, inc=1, device_id=(s, r, lax.rem(c + k, cols)), device_id_type=MESH
        )
        greeted += 1
    for k in range(1, row_count):
        pl.semaphore_signal(
            barrier, inc=1, device_id=(s, lax.rem(r + k, row_count), c), device_id_type=MESH
        )
        greeted += 1
    for step in (1, sections - 1):
        for other in range(row_count):
            pl.semaphore_signal(
                barrier,
                inc=1,
                device_id=(lax.rem(s + step, sections), other, c),
                device_id_type=MESH,
            )
            greeted += 1

    to_row = lax.broadcasted_iota(jnp.int32, (rows, rows), 0)
    from_row = lax.broadcasted_iota(jnp.int32, (rows, rows), 1)
    order = jnp.zeros((rows, rows), jnp.bool_)
    back = jnp.zeros((rows, rows), jnp.bool_)
    for at in range(cols):
        for m in range(micro):
            first, source = at * own + m * seq_part, m * batch + at * seq_part
            inside = (to_row >= first) & (to_row < first + seq_part)
            order = order | (inside & (to_row - from_row == first - source))
            inside = (from_row >= first) & (from_row < first + seq_part)
            back = back | (inside & (from_row - to_row == first - source))
    order = jnp.where(order, 1.0, 0.0).astype(jnp.bfloat16)
    back = jnp.where(back, 1.0, 0.0).astype(jnp.bfloat16)

    row_at = lax.broadcasted_iota(jnp.int32, (own, head_dim), 0)
    lane = lax.broadcasted_iota(jnp.int32, (own, head_dim), 1)
    half = head_dim // 2
    half_lane = jnp.where(lane < half, lane, lane - half).astype(jnp.float32)
    frequency = jnp.exp(half_lane * (-2.0 * math.log(500000.0) / head_dim))
    length_of, cosines, sines = [], [], []
    for lot in range(lots):
        position = jnp.zeros((own, head_dim), jnp.float32)
        length_of.append([])
        for i in range(own):
            length = lengths[i % seq_part, lot * micro + i // seq_part]
            length_of[lot].append(length)
            position = jnp.where(row_at == i, length.astype(jnp.float32), position)
        angles = position * frequency
        cosines.append(jnp.cos(angles))
        sine = jnp.sin(angles)
        sines.append(jnp.where(lane < half, -sine, sine))

    head_at = lax.broadcasted_iota(jnp.int32, (heads, spots), 0)
    spot_at = lax.broadcasted_iota(jnp.int32, (heads, spots), 1)
    head_group = jnp.zeros((heads, spots), jnp.int32)
    for g in range(1, groups):
        head_group = head_group + jnp.where(head_at >= g * per, 1, 0)
    same_group = remainder(spot_at, groups) == head_group

    pl.semaphore_wait(barrier, greeted)

    copies = []
    square_copies, part_copies, attended_copies = [], [], []
    for lot in range(lots):
        @pl.when(s == 0)
        def _():
            entry = hidden[lot * micro : (lot + 1) * micro].astype(jnp.float32)
            entry = entry.reshape(rows, depth).astype(jnp.bfloat16)
            state[lot] = jnp.dot(order, entry, preferred_element_type=jnp.float32)

        @pl.when(s > 0)
        def _():
            for n in range(pieces):
                for other in range(row_count):
                    remote(
                        mixed.at[lot, 0, n],
                        arrived.at[lot, other, n],
                        x_send.at[lot, n, 0],
                        x_recv.at[lot, n, other],
                        (s, r, c),
                    ).wait_recv()
                total = arrived[lot, 0, n]
                for other in range(1, row_count):
                    total = total + arrived[lot, other, n]
                state[lot, :, n * piece : (n + 1) * piece] = total.astype(jnp.bfloat16).astype(
                    jnp.float32
                )

        current = state[lot]
        squares = jnp.sum(current * current, axis=1, keepdims=True)
        squares = jnp.broadcast_to(squares, (rows, head_dim))
        for at in range(cols):
            square[lot, at] = squares[at * own : (at + 1) * own]
        started = []
        for k in range(1, cols):
            peer = lax.rem(c + k, cols)
            started.append(
                remote(
                    square.at[lot, peer],
                    square_in.at[lot, k - 1],
                    sq_send.at[lot, k - 1],
                    sq_recv.at[lot, k - 1],
                    (s, r, peer),
                )
            )
            started[-1].start()
        square_copies.append(started)
        copies += started
        scaled = (current * gain[...].astype(jnp.float32)).astype(jnp.bfloat16)
        part_copies.append([])
        for g in range(groups):
            if lot == 0:
                loads[g].wait()
            product = jnp.dot(scaled, wq[g], preferred_element_type=jnp.float32)
            for at in range(cols):
                part[lot, g, at] = product[at * own : (at + 1) * own]
            started = []
            for k in range(1, cols):
                peer = lax.rem(c + k, cols)
                started.append(
                    remote(
                        part.at[lot, g, peer],
                        part_in.at[lot, g, k - 1],
                        rs_send.at[lot, g, k - 1],
                        rs_recv.at[lot, g, k - 1],
                        (s, r, peer),
                    )
                )
                started[-1].start()
            part_copies[lot].append(started)
            copies += started

    load_keys.wait()
    load_values.wait()
    scale = 1.0 / math.sqrt(head_dim)
    seqs = range(own)
    for lot in range(lots):

        def rotate(vectors):
            return vectors * cosines[lot] + pltpu.roll(vectors, half, 1) * sines[lot]

        for copy in square_copies[lot]:
            copy.wait_recv()
        total = square[lot, c]
        for k in range(1, cols):
            total = total + square_in[lot, k - 1]
        factor = lax.rsqrt(total / D + 1e-05)
        for g in range(groups):
            for copy in part_copies[lot][g]:
                copy.wait_recv()
            total = part[lot, g, c]
            for k in range(1, cols):
                total = total + part_in[lot, g, k - 1]
            cut = [total[:, i * head_dim : (i + 1) * head_dim] * factor for i in range(per + 2)]
            new_key = rotate(cut[per]).astype(jnp.bfloat16).astype(jnp.float32)
            new_value = cut[per + 1].astype(jnp.bfloat16).astype(jnp.float32)
            for i in range(per):
                at = pl.ds((g * per + i) * own, own)
                q_rows[lot, at, :] = rotate(cut[i])
                k_rows[lot, at, :] = new_key
                v_rows[lot, at, :] = new_value
        taken = [pl.ds(i, heads, stride=own) for i in seqs]
        queries = [q_rows[lot, taken[i], :].astype(jnp.bfloat16) for i in seqs]
        scores = [
            lax.dot_general(
                queries[i],
                keys[lot * own + i],
                (((1,), (1,)), ((), ())),
                preferred_element_type=jnp.float32,
            )
            * scale
            for i in seqs
        ]
        own_scores = [
            jnp.sum(
                queries[i].astype(jnp.float32) * k_rows[lot, taken[i], :], axis=1, keepdims=True
            )
            * scale
            for i in seqs
        ]
        weights, own_weights = [], []
        for i in seqs:
            visible = same_group & (spot_at < length_of[lot][i] * groups)
            masked = jnp.where(visible, scores[i], -jnp.inf)
            row_max = jnp.maximum(jnp.max(masked, axis=1, keepdims=True), own_scores[i])
            cache_exp = jnp.exp(masked - row_max)
            own_exp = jnp.exp(own_scores[i] - row_max)
            total = jnp.sum(cache_exp, axis=1, keepdims=True) + own_exp
            weights.append((cache_exp / total).astype(jnp.bfloat16))
            own_weights.append((own_exp / total).astype(jnp.bfloat16).astype(jnp.float32))
        for i in seqs:
            result = jnp.dot(
                weights[i], values[lot * own + i], preferred_element_type=jnp.float32
            )
            a_rows[lot, taken[i], :] = result + own_weights[i] * v_rows[lot, taken[i], :]
        for h in range(heads):
            attended[lot, c, :, h * head_dim : (h + 1) * head_dim] = a_rows[
                lot, h * own : (h + 1) * own, :
            ].astype(jnp.bfloat16)
        started = []
        for k in range(1, cols):
            peer = lax.rem(c + k, cols)
            started.append(
                remote(
                    attended.at[lot, c],
                    attended.at[lot, c],
                    at_send.at[lot, k - 1],
                    at_recv.at[lot, k - 1],
                    (s, r, peer),
                )
            )
            started[-1].start()
        attended_copies.append(started)
        copies += started

    load_wo.wait()

    def onward(lot, n, other):
        return remote(
            mixed.at[lot, r, n],
            arrived.at[lot, r, n],
            x_send.at[lot, n, other],
            x_recv.at[lot, n, r],
            (lax.rem(s + 1, sections), other, c),
        )

    def sideways(lot, n, k):
        return remote(
            mixed.at[lot, r, n],
            mixed.at[lot, r, n],
            y_send.at[lot, n, k - 1],
            y_recv.at[lot, n, k - 1],
            (s, lax.rem(r + k, row_count), c),
        )

    for lot in range(lots):
        for copy in attended_copies[lot]:
            copy.wait_recv()
        for at in range(cols):
            gathered[lot, at * own : (at + 1) * own, :] = attended[lot, at].astype(jnp.float32)
        everyone = gathered[lot].astype(jnp.bfloat16)
        for n in range(pieces):
            at = slice(n * piece, (n + 1) * piece)
            product = jnp.dot(everyone, wo[:, at], preferred_element_type=jnp.float32)
            mixed[lot, r, n] = product + jnp.where(r == 0, state[lot, :, at], 0.0)

            @pl.when(s < sections - 1)
            def _():
                for other in range(row_count):
                    onward(lot, n, other).start()

            @pl.when(s == sections - 1)
            def _():
                for k in range(1, row_count):
                    sideways(lot, n, k).start()

    @pl.when(s < sections - 1)
    def _():
        for lot in range(lots):
            for n in range(pieces):
                for k in range(1, row_count):
                    sideways(lot, n, k).start()

    for lot in range(lots):
        for n in range(pieces):
            for k in range(1, row_count):
                sideways(lot, n, k).wait_recv()
            total = mixed[lot, 0, n]
            for other in range(1, row_count):
                total = total + mixed[lot, other, n]
            final = jnp.dot(back, total.astype(jnp.bfloat16), preferred_element_type=jnp.float32)
            out[lot * micro : (lot + 1) * micro, :, n * piece : (n + 1) * piece] = final.reshape(
                micro, batch, piece
            ).astype(jnp.bfloat16)

    for copy in copies:
        copy.wait_send()
    for lot in range(lots):
        for n in range(pieces):
            for k in range(1, row_count):
                sideways(lot, n, k).wait_send()

    @pl.when(s < sections - 1)
    def _():
        for lot in range(lots):
            for n in range(pieces):
                for other in range(row_count):
                    onward(lot, n, other).wait_send()


def shards(hidden, norm_gain, w_qkv, w_out, cache_keys, cache_values, cache_lengths):
    sections, row_count, cols = (lax.axis_size(a) for a in ("section", "row", "col"))
    micro, batch, depth = hidden.shape
    rows = micro // LOTS * batch
    own = rows // cols
    spots, groups, head_dim = cache_keys.shape[3:]
    per = HEADS // KVH
    heads = groups * per
    chunk = (per + 2) * head_dim
    piece = min(256, w_out.shape[2])
    pieces = w_out.shape[2] // piece
    keys = cache_keys.reshape(LOTS * own, spots * groups, head_dim)
    values = cache_values.reshape(LOTS * own, spots * groups, head_dim)
    vmem = pl.BlockSpec(memory_space=pltpu.VMEM)
    hbm = pl.BlockSpec(memory_space=pl.ANY)
    dma = pltpu.SemaphoreType.DMA
    f32, bf16 = jnp.float32, jnp.bfloat16
    return pl.pallas_call(
        functools.partial(kernel, (sections, row_count, cols)),
        out_shape=jax.ShapeDtypeStruct((micro, batch, depth), bf16),
        in_specs=[vmem, vmem, hbm, hbm, hbm, hbm, pl.BlockSpec(memory_space=pltpu.SMEM)],
        out_specs=vmem,
        scratch_shapes=[
            pltpu.VMEM((groups, depth, chunk), bf16),
            pltpu.VMEM(w_out.shape[1:], bf16),
            pltpu.VMEM(keys.shape, bf16),
            pltpu.VMEM(values.shape, bf16),
            pltpu.VMEM((LOTS, rows, depth), f32),
            pltpu.VMEM((LOTS, groups, cols, own, chunk), f32),
            pltpu.VMEM((LOTS, groups, cols - 1, own, chunk), f32),
            pltpu.VMEM((LOTS, cols, own, head_dim), f32),
            pltpu.VMEM((LOTS, cols - 1, own, head_dim), f32),
            pltpu.VMEM((LOTS, heads * own, head_dim), f32),
            pltpu.VMEM((LOTS, heads * own, head_dim), f32),
            pltpu.VMEM((LOTS, heads * own, head_dim), f32),
            pltpu.VMEM((LOTS, heads * own, head_dim), f32),
            pltpu.VMEM((LOTS, cols, own, heads * head_dim), bf16),
            pltpu.VMEM((LOTS, rows, heads * head_dim), f32),
            pltpu.VMEM((LOTS, row_count, pieces, rows, piece), f32),
            pltpu.VMEM((LOTS, row_count, pieces, rows, piece), f32),
            dma((groups + 3,)),
            dma((LOTS, groups, cols - 1)),
            dma((LOTS, groups, cols - 1)),
            dma((LOTS, cols - 1)),
            dma((LOTS, cols - 1)),
            dma((LOTS, cols - 1)),
            dma((LOTS, cols - 1)),
            dma((LOTS, pieces, row_count)),
            dma((LOTS, pieces, row_count)),
            dma((LOTS, pieces, row_count - 1)),
            dma((LOTS, pieces, row_count - 1)),
        ],
        compiler_params=pltpu.CompilerParams(collective_id=0, has_side_effects=True),
    )(hidden, norm_gain, w_qkv[0], w_out[0], keys, values, cache_lengths.T)[None]


def solution(mesh):
    return jax.shard_map(
        shards,
        mesh=mesh,
        in_specs=(
            P(None, None, "col"),
            P("section", "col"),
            P("section", "col", "row"),
            P("section", "row", "col"),
            P("section", None, "col", None, "row", None),
            P("section", None, "col", None, "row", None),
            P(None, "col"),
        ),
        out_specs=P("section", None, None, "col"),
        check_vma=False,
    )
```

```python
import functools
import math

import jax
import jax.numpy as jnp
from jax import lax
from jax.experimental import pallas as pl
from jax.experimental.pallas import tpu as pltpu
from jax.sharding import PartitionSpec as P

D = 4096
HEADS = 32
KVH = 8
LOTS = 4
MESH = pl.DeviceIdType.MESH


def remainder(values, by):
    if by & (by - 1) == 0:
        return values & (by - 1)
    return lax.rem(values, jnp.full_like(values, by))


def kernel(
    dims,
    hidden,
    gain,
    wq_hbm,
    wo_hbm,
    keys_hbm,
    values_hbm,
    lengths,
    out,
    wq,
    wo,
    keys,
    values,
    state,
    part,
    part_in,
    square,
    square_in,
    q_rows,
    k_rows,
    v_rows,
    a_rows,
    attended,
    gathered,
    mixed,
    arrived,
    load_sem,
    rs_send,
    rs_recv,
    sq_send,
    sq_recv,
    at_send,
    at_recv,
    x_send,
    x_recv,
    y_send,
    y_recv,
):
    sections, row_count, cols = dims
    s = lax.axis_index("section")
    r = lax.axis_index("row")
    c = lax.axis_index("col")
    batch, depth = hidden.shape[1:]
    lots, rows = state.shape[:2]
    micro = rows // batch
    own = rows // cols
    seq_part = batch // cols
    groups, chunk = wq.shape[0], wq.shape[2]
    head_dim = keys.shape[2]
    per = HEADS // KVH
    heads = groups * per
    spots = keys.shape[1]
    pieces, piece = mixed.shape[2], mixed.shape[4]

    def remote(src, dst, send_sem, recv_sem, device):
        return pltpu.make_async_remote_copy(
            src_ref=src,
            dst_ref=dst,
            send_sem=send_sem,
            recv_sem=recv_sem,
            device_id=device,
            device_id_type=MESH,
        )

    loads = [
        pltpu.make_async_copy(
            wq_hbm.at[:, pl.ds(g * chunk, chunk)], wq.at[g], load_sem.at[g]
        )
        for g in range(groups)
    ]
    load_keys = pltpu.make_async_copy(keys_hbm, keys, load_sem.at[groups])
    load_values = pltpu.make_async_copy(values_hbm, values, load_sem.at[groups + 1])
    load_wo = pltpu.make_async_copy(wo_hbm, wo, load_sem.at[groups + 2])
    for load in loads + [load_keys, load_values, load_wo]:
        load.start()

    barrier = pltpu.get_barrier_semaphore()
    greeted = 0
    for k in range(1, cols):
        pl.semaphore_signal(
            barrier, inc=1, device_id=(s, r, lax.rem(c + k, cols)), device_id_type=MESH
        )
        greeted += 1
    for k in range(1, row_count):
        pl.semaphore_signal(
            barrier, inc=1, device_id=(s, lax.rem(r + k, row_count), c), device_id_type=MESH
        )
        greeted += 1
    for step in (1, sections - 1):
        for other in range(row_count):
            pl.semaphore_signal(
                barrier,
                inc=1,
                device_id=(lax.rem(s + step, sections), other, c),
                device_id_type=MESH,
            )
            greeted += 1

    to_row = lax.broadcasted_iota(jnp.int32, (rows, rows), 0)
    from_row = lax.broadcasted_iota(jnp.int32, (rows, rows), 1)
    order = jnp.zeros((rows, rows), jnp.bool_)
    back = jnp.zeros((rows, rows), jnp.bool_)
    for at in range(cols):
        for m in range(micro):
            first, source = at * own + m * seq_part, m * batch + at * seq_part
            inside = (to_row >= first) & (to_row < first + seq_part)
            order = order | (inside & (to_row - from_row == first - source))
            inside = (from_row >= first) & (from_row < first + seq_part)
            back = back | (inside & (from_row - to_row == first - source))
    order = jnp.where(order, 1.0, 0.0).astype(jnp.bfloat16)
    back = jnp.where(back, 1.0, 0.0).astype(jnp.bfloat16)

    row_at = lax.broadcasted_iota(jnp.int32, (own, head_dim), 0)
    lane = lax.broadcasted_iota(jnp.int32, (own, head_dim), 1)
    half = head_dim // 2
    half_lane = jnp.where(lane < half, lane, lane - half).astype(jnp.float32)
    frequency = jnp.exp(half_lane * (-2.0 * math.log(500000.0) / head_dim))
    length_of, cosines, sines = [], [], []
    for lot in range(lots):
        position = jnp.zeros((own, head_dim), jnp.float32)
        length_of.append([])
        for i in range(own):
            length = lengths[i % seq_part, lot * micro + i // seq_part]
            length_of[lot].append(length)
            position = jnp.where(row_at == i, length.astype(jnp.float32), position)
        angles = position * frequency
        cosines.append(jnp.cos(angles))
        sine = jnp.sin(angles)
        sines.append(jnp.where(lane < half, -sine, sine))

    head_at = lax.broadcasted_iota(jnp.int32, (heads, spots), 0)
    spot_at = lax.broadcasted_iota(jnp.int32, (heads, spots), 1)
    head_group = jnp.zeros((heads, spots), jnp.int32)
    for g in range(1, groups):
        head_group = head_group + jnp.where(head_at >= g * per, 1, 0)
    same_group = remainder(spot_at, groups) == head_group

    pl.semaphore_wait(barrier, greeted)

    copies = []
    square_copies, part_copies, attended_copies = [], [], []
    for lot in range(lots):
        @pl.when(s == 0)
        def _():
            entry = hidden[lot * micro : (lot + 1) * micro].astype(jnp.float32)
            entry = entry.reshape(rows, depth).astype(jnp.bfloat16)
            state[lot] = jnp.dot(order, entry, preferred_element_type=jnp.float32)

        @pl.when(s > 0)
        def _():
            for n in range(pieces):
                for other in range(row_count):
                    remote(
                        mixed.at[lot, 0, n],
                        arrived.at[lot, other, n],
                        x_send.at[lot, n, 0],
                        x_recv.at[lot, n, other],
                        (s, r, c),
                    ).wait_recv()
                total = arrived[lot, 0, n]
                for other in range(1, row_count):
                    total = total + arrived[lot, other, n]
                state[lot, :, n * piece : (n + 1) * piece] = total.astype(jnp.bfloat16).astype(
                    jnp.float32
                )

        current = state[lot]
        squares = jnp.sum(current * current, axis=1, keepdims=True)
        squares = jnp.broadcast_to(squares, (rows, head_dim))
        for at in range(cols):
            square[lot, at] = squares[at * own : (at + 1) * own]
        started = []
        for k in range(1, cols):
            peer = lax.rem(c + k, cols)
            started.append(
                remote(
                    square.at[lot, peer],
                    square_in.at[lot, k - 1],
                    sq_send.at[lot, k - 1],
                    sq_recv.at[lot, k - 1],
                    (s, r, peer),
                )
            )
            started[-1].start()
        square_copies.append(started)
        copies += started
        scaled = (current * gain[...].astype(jnp.float32)).astype(jnp.bfloat16)
        part_copies.append([])
        for g in range(groups):
            if lot == 0:
                loads[g].wait()
            product = jnp.dot(scaled, wq[g], preferred_element_type=jnp.float32)
            for at in range(cols):
                part[lot, g, at] = product[at * own : (at + 1) * own]
            started = []
            for k in range(1, cols):
                peer = lax.rem(c + k, cols)
                started.append(
                    remote(
                        part.at[lot, g, peer],
                        part_in.at[lot, g, k - 1],
                        rs_send.at[lot, g, k - 1],
                        rs_recv.at[lot, g, k - 1],
                        (s, r, peer),
                    )
                )
                started[-1].start()
            part_copies[lot].append(started)
            copies += started

    load_keys.wait()
    load_values.wait()
    scale = 1.0 / math.sqrt(head_dim)
    seqs = range(own)
    for lot in range(lots):

        def rotate(vectors):
            return vectors * cosines[lot] + pltpu.roll(vectors, half, 1) * sines[lot]

        for copy in square_copies[lot]:
            copy.wait_recv()
        total = square[lot, c]
        for k in range(1, cols):
            total = total + square_in[lot, k - 1]
        factor = lax.rsqrt(total / D + 1e-05)
        for g in range(groups):
            for copy in part_copies[lot][g]:
                copy.wait_recv()
            total = part[lot, g, c]
            for k in range(1, cols):
                total = total + part_in[lot, g, k - 1]
            cut = [total[:, i * head_dim : (i + 1) * head_dim] * factor for i in range(per + 2)]
            new_key = rotate(cut[per]).astype(jnp.bfloat16).astype(jnp.float32)
            new_value = cut[per + 1].astype(jnp.bfloat16).astype(jnp.float32)
            for i in range(per):
                at = pl.ds((g * per + i) * own, own)
                q_rows[lot, at, :] = rotate(cut[i])
                k_rows[lot, at, :] = new_key
                v_rows[lot, at, :] = new_value
        taken = [pl.ds(i, heads, stride=own) for i in seqs]
        queries = [q_rows[lot, taken[i], :].astype(jnp.bfloat16) for i in seqs]
        scores = [
            lax.dot_general(
                queries[i],
                keys[lot * own + i],
                (((1,), (1,)), ((), ())),
                preferred_element_type=jnp.float32,
            )
            * scale
            for i in seqs
        ]
        own_scores = [
            jnp.sum(
                queries[i].astype(jnp.float32) * k_rows[lot, taken[i], :], axis=1, keepdims=True
            )
            * scale
            for i in seqs
        ]
        weights, own_weights = [], []
        for i in seqs:
            visible = same_group & (spot_at < length_of[lot][i] * groups)
            masked = jnp.where(visible, scores[i], -jnp.inf)
            row_max = jnp.maximum(jnp.max(masked, axis=1, keepdims=True), own_scores[i])
            cache_exp = jnp.exp(masked - row_max)
            own_exp = jnp.exp(own_scores[i] - row_max)
            total = jnp.sum(cache_exp, axis=1, keepdims=True) + own_exp
            weights.append((cache_exp / total).astype(jnp.bfloat16))
            own_weights.append((own_exp / total).astype(jnp.bfloat16).astype(jnp.float32))
        for i in seqs:
            result = jnp.dot(
                weights[i], values[lot * own + i], preferred_element_type=jnp.float32
            )
            a_rows[lot, taken[i], :] = result + own_weights[i] * v_rows[lot, taken[i], :]
        for h in range(heads):
            attended[lot, c, :, h * head_dim : (h + 1) * head_dim] = a_rows[
                lot, h * own : (h + 1) * own, :
            ].astype(jnp.bfloat16)
        started = []
        for k in range(1, cols):
            peer = lax.rem(c + k, cols)
            started.append(
                remote(
                    attended.at[lot, c],
                    attended.at[lot, c],
                    at_send.at[lot, k - 1],
                    at_recv.at[lot, k - 1],
                    (s, r, peer),
                )
            )
            started[-1].start()
        attended_copies.append(started)
        copies += started

    load_wo.wait()

    def onward(lot, n, other):
        return remote(
            mixed.at[lot, r, n],
            arrived.at[lot, r, n],
            x_send.at[lot, n, other],
            x_recv.at[lot, n, r],
            (lax.rem(s + 1, sections), other, c),
        )

    def sideways(lot, n, k):
        return remote(
            mixed.at[lot, r, n],
            mixed.at[lot, r, n],
            y_send.at[lot, n, k - 1],
            y_recv.at[lot, n, k - 1],
            (s, lax.rem(r + k, row_count), c),
        )

    for lot in range(lots):
        for copy in attended_copies[lot]:
            copy.wait_recv()
        for at in range(cols):
            gathered[lot, at * own : (at + 1) * own, :] = attended[lot, at].astype(jnp.float32)
        everyone = gathered[lot].astype(jnp.bfloat16)
        for n in range(pieces):
            at = slice(n * piece, (n + 1) * piece)
            product = jnp.dot(everyone, wo[:, at], preferred_element_type=jnp.float32)
            mixed[lot, r, n] = product + jnp.where(r == 0, state[lot, :, at], 0.0)

            @pl.when(s < sections - 1)
            def _():
                for other in range(row_count):
                    onward(lot, n, other).start()

            @pl.when(s == sections - 1)
            def _():
                for k in range(1, row_count):
                    sideways(lot, n, k).start()

    @pl.when(s < sections - 1)
    def _():
        for lot in range(lots):
            for n in range(pieces):
                for k in range(1, row_count):
                    sideways(lot, n, k).start()

    for lot in range(lots):
        for n in range(pieces):
            for k in range(1, row_count):
                sideways(lot, n, k).wait_recv()
            total = mixed[lot, 0, n]
            for other in range(1, row_count):
                total = total + mixed[lot, other, n]
            final = jnp.dot(back, total.astype(jnp.bfloat16), preferred_element_type=jnp.float32)
            out[lot * micro : (lot + 1) * micro, :, n * piece : (n + 1) * piece] = final.reshape(
                micro, batch, piece
            ).astype(jnp.bfloat16)

    for copy in copies:
        copy.wait_send()
    for lot in range(lots):
        for n in range(pieces):
            for k in range(1, row_count):
                sideways(lot, n, k).wait_send()

    @pl.when(s < sections - 1)
    def _():
        for lot in range(lots):
            for n in range(pieces):
                for other in range(row_count):
                    onward(lot, n, other).wait_send()


def shards(hidden, norm_gain, w_qkv, w_out, cache_keys, cache_values, cache_lengths):
    sections, row_count, cols = (lax.axis_size(a) for a in ("section", "row", "col"))
    micro, batch, depth = hidden.shape
    rows = micro // LOTS * batch
    own = rows // cols
    spots, groups, head_dim = cache_keys.shape[3:]
    per = HEADS // KVH
    heads = groups * per
    chunk = (per + 2) * head_dim
    piece = min(256, w_out.shape[2])
    pieces = w_out.shape[2] // piece
    keys = cache_keys.reshape(LOTS * own, spots * groups, head_dim)
    values = cache_values.reshape(LOTS * own, spots * groups, head_dim)
    vmem = pl.BlockSpec(memory_space=pltpu.VMEM)
    hbm = pl.BlockSpec(memory_space=pl.ANY)
    dma = pltpu.SemaphoreType.DMA
    f32, bf16 = jnp.float32, jnp.bfloat16
    return pl.pallas_call(
        functools.partial(kernel, (sections, row_count, cols)),
        out_shape=jax.ShapeDtypeStruct((micro, batch, depth), bf16),
        in_specs=[vmem, vmem, hbm, hbm, hbm, hbm, pl.BlockSpec(memory_space=pltpu.SMEM)],
        out_specs=vmem,
        scratch_shapes=[
            pltpu.VMEM((groups, depth, chunk), bf16),
            pltpu.VMEM(w_out.shape[1:], bf16),
            pltpu.VMEM(keys.shape, bf16),
            pltpu.VMEM(values.shape, bf16),
            pltpu.VMEM((LOTS, rows, depth), f32),
            pltpu.VMEM((LOTS, groups, cols, own, chunk), f32),
            pltpu.VMEM((LOTS, groups, cols - 1, own, chunk), f32),
            pltpu.VMEM((LOTS, cols, own, head_dim), f32),
            pltpu.VMEM((LOTS, cols - 1, own, head_dim), f32),
            pltpu.VMEM((LOTS, heads * own, head_dim), f32),
            pltpu.VMEM((LOTS, heads * own, head_dim), f32),
            pltpu.VMEM((LOTS, heads * own, head_dim), f32),
            pltpu.VMEM((LOTS, heads * own, head_dim), f32),
            pltpu.VMEM((LOTS, cols, own, heads * head_dim), bf16),
            pltpu.VMEM((LOTS, rows, heads * head_dim), f32),
            pltpu.VMEM((LOTS, row_count, pieces, rows, piece), f32),
            pltpu.VMEM((LOTS, row_count, pieces, rows, piece), f32),
            dma((groups + 3,)),
            dma((LOTS, groups, cols - 1)),
            dma((LOTS, groups, cols - 1)),
            dma((LOTS, cols - 1)),
            dma((LOTS, cols - 1)),
            dma((LOTS, cols - 1)),
            dma((LOTS, cols - 1)),
            dma((LOTS, pieces, row_count)),
            dma((LOTS, pieces, row_count)),
            dma((LOTS, pieces, row_count - 1)),
            dma((LOTS, pieces, row_count - 1)),
        ],
        compiler_params=pltpu.CompilerParams(collective_id=0, has_side_effects=True),
    )(hidden, norm_gain, w_qkv[0], w_out[0], keys, values, cache_lengths.T)[None]


def solution(mesh):
    return jax.shard_map(
        shards,
        mesh=mesh,
        in_specs=(
            P(None, None, "col"),
            P("section", "col"),
            P("section", "col", "row"),
            P("section", "row", "col"),
            P("section", None, "col", None, "row", None),
            P("section", None, "col", None, "row", None),
            P(None, "col"),
        ),
        out_specs=P("section", None, None, "col"),
        check_vma=False,
    )
```

```python
import functools
import math

import jax
import jax.numpy as jnp
from jax import lax
from jax.experimental import pallas as pl
from jax.experimental.pallas import tpu as pltpu
from jax.sharding import PartitionSpec as P

D = 4096
HEADS = 32
KVH = 8
LOTS = 2
CUTS = 4
PIECE = 512
MESH = pl.DeviceIdType.MESH


def remainder(values, by):
    if by & (by - 1) == 0:
        return values & (by - 1)
    return lax.rem(values, jnp.full_like(values, by))


def kernel(
    dims,
    hidden_hbm,
    gain_hbm,
    wq_hbm,
    wo_hbm,
    keys_hbm,
    values_hbm,
    lengths_hbm,
    out,
    hidden,
    gain,
    lengths,
    wq,
    wo,
    keys,
    values,
    state,
    part,
    part_in,
    q_rows,
    k_rows,
    v_rows,
    a_rows,
    attended,
    gathered,
    mixed,
    arrived,
    load_sem,
    rs_send,
    rs_recv,
    at_send,
    at_recv,
    x_send,
    x_recv,
    y_send,
    y_recv,
):
    sections, row_count, cols = dims
    s = lax.axis_index("section")
    r = lax.axis_index("row")
    c = lax.axis_index("col")
    batch, depth = hidden.shape[1:]
    lots, rows = state.shape[:2]
    micro = rows // batch
    own = rows // cols
    seq_part = batch // cols
    groups, chunk = wq.shape[0], wq.shape[2]
    head_dim = keys.shape[2]
    per = HEADS // KVH
    heads = groups * per
    spots = keys.shape[1]
    pieces, piece = mixed.shape[2], mixed.shape[4]
    cuts = part.shape[1]
    grouped = groups // cuts
    width = grouped * chunk

    def remote(src, dst, send_sem, recv_sem, device):
        return pltpu.make_async_remote_copy(
            src_ref=src,
            dst_ref=dst,
            send_sem=send_sem,
            recv_sem=recv_sem,
            device_id=device,
            device_id_type=MESH,
        )

    loads = [
        pltpu.make_async_copy(
            wq_hbm.at[:, pl.ds(g * chunk, chunk)], wq.at[g], load_sem.at[g]
        )
        for g in range(groups)
    ]
    load_keys = pltpu.make_async_copy(keys_hbm, keys, load_sem.at[groups])
    load_values = pltpu.make_async_copy(values_hbm, values, load_sem.at[groups + 1])
    load_wo = pltpu.make_async_copy(wo_hbm, wo, load_sem.at[groups + 2])
    load_lengths = pltpu.make_async_copy(lengths_hbm, lengths, load_sem.at[groups + 3])
    load_hidden = pltpu.make_async_copy(hidden_hbm, hidden, load_sem.at[groups + 4])
    load_gain = pltpu.make_async_copy(gain_hbm, gain, load_sem.at[groups + 5])
    for load in [load_lengths, load_hidden, load_gain] + loads + [load_keys, load_values, load_wo]:
        load.start()

    barrier = pltpu.get_barrier_semaphore()
    greeted = 0
    for k in range(1, cols):
        pl.semaphore_signal(
            barrier, inc=1, device_id=(s, r, lax.rem(c + k, cols)), device_id_type=MESH
        )
        greeted += 1
    for k in range(1, row_count):
        pl.semaphore_signal(
            barrier, inc=1, device_id=(s, lax.rem(r + k, row_count), c), device_id_type=MESH
        )
        greeted += 1
    for step in (1, sections - 1):
        for other in range(row_count):
            pl.semaphore_signal(
                barrier,
                inc=1,
                device_id=(lax.rem(s + step, sections), other, c),
                device_id_type=MESH,
            )
            greeted += 1

    to_row = lax.broadcasted_iota(jnp.int32, (rows, rows), 0)
    from_row = lax.broadcasted_iota(jnp.int32, (rows, rows), 1)
    order = jnp.zeros((rows, rows), jnp.bool_)
    back = jnp.zeros((rows, rows), jnp.bool_)
    for at in range(cols):
        for m in range(micro):
            first, source = at * own + m * seq_part, m * batch + at * seq_part
            inside = (to_row >= first) & (to_row < first + seq_part)
            order = order | (inside & (to_row - from_row == first - source))
            inside = (from_row >= first) & (from_row < first + seq_part)
            back = back | (inside & (from_row - to_row == first - source))
    order = jnp.where(order, 1.0, 0.0).astype(jnp.bfloat16)
    back = jnp.where(back, 1.0, 0.0).astype(jnp.bfloat16)

    row_at = lax.broadcasted_iota(jnp.int32, (own, head_dim), 0)
    lane = lax.broadcasted_iota(jnp.int32, (own, head_dim), 1)
    half = head_dim // 2
    half_lane = jnp.where(lane < half, lane, lane - half).astype(jnp.float32)
    frequency = jnp.exp(half_lane * (-2.0 * math.log(500000.0) / head_dim))
    load_lengths.wait()
    length_of, cosines, sines = [], [], []
    for lot in range(lots):
        position = jnp.zeros((own, head_dim), jnp.float32)
        length_of.append([])
        for i in range(own):
            length = lengths[i % seq_part, lot * micro + i // seq_part]
            length_of[lot].append(length)
            position = jnp.where(row_at == i, length.astype(jnp.float32), position)
        angles = position * frequency
        cosines.append(jnp.cos(angles))
        sine = jnp.sin(angles)
        sines.append(jnp.where(lane < half, -sine, sine))

    head_at = lax.broadcasted_iota(jnp.int32, (heads, spots), 0)
    spot_at = lax.broadcasted_iota(jnp.int32, (heads, spots), 1)
    head_group = jnp.zeros((heads, spots), jnp.int32)
    for g in range(1, groups):
        head_group = head_group + jnp.where(head_at >= g * per, 1, 0)
    same_group = remainder(spot_at, groups) == head_group

    load_hidden.wait()
    load_gain.wait()

    @pl.when(s == 0)
    def _():
        for lot in range(lots):
            entry = hidden[lot * micro : (lot + 1) * micro].astype(jnp.float32)
            entry = entry.reshape(rows, depth).astype(jnp.bfloat16)
            state[lot] = jnp.dot(order, entry, preferred_element_type=jnp.float32)

    pl.semaphore_wait(barrier, greeted)

    copies = []
    part_copies, attended_copies = [], []
    for lot in range(lots):
        @pl.when(s > 0)
        def _():
            for n in range(pieces):
                for other in range(row_count):
                    remote(
                        mixed.at[lot, 0, n],
                        arrived.at[lot, other, n],
                        x_send.at[lot, n, 0],
                        x_recv.at[lot, n, other],
                        (s, r, c),
                    ).wait_recv()
                total = arrived[lot, 0, n]
                for other in range(1, row_count):
                    total = total + arrived[lot, other, n]
                state[lot, :, n * piece : (n + 1) * piece] = total.astype(jnp.bfloat16).astype(
                    jnp.float32
                )

        current = state[lot]
        squares = jnp.sum(current * current, axis=1, keepdims=True)
        squares = jnp.broadcast_to(squares, (rows, head_dim))
        for at in range(cols):
            part[lot, 0, at, :, width:] = squares[at * own : (at + 1) * own]
        scaled = (current * gain[...].astype(jnp.float32)).astype(jnp.bfloat16)
        part_copies.append([])
        for g in range(groups):
            if lot == 0:
                loads[g].wait()
            product = jnp.dot(scaled, wq[g], preferred_element_type=jnp.float32)
            cut, at_lane = g // grouped, g % grouped * chunk
            for at in range(cols):
                part[lot, cut, at, :, at_lane : at_lane + chunk] = product[
                    at * own : (at + 1) * own
                ]
            if (g + 1) % grouped:
                continue
            started = []
            sent = pl.ds(0, width + head_dim if cut == 0 else width)
            for k in range(1, cols):
                peer = lax.rem(c + k, cols)
                started.append(
                    remote(
                        part.at[lot, cut, peer, :, sent],
                        part_in.at[lot, cut, k - 1, :, sent],
                        rs_send.at[lot, cut, k - 1],
                        rs_recv.at[lot, cut, k - 1],
                        (s, r, peer),
                    )
                )
                started[-1].start()
            part_copies[lot].append(started)
            copies += started

    load_keys.wait()
    load_values.wait()
    scale = 1.0 / math.sqrt(head_dim)
    seqs = range(own)
    for lot in range(lots):

        def rotate(vectors):
            return vectors * cosines[lot] + pltpu.roll(vectors, half, 1) * sines[lot]

        for g in range(groups):
            cut, lanes = g // grouped, slice(g % grouped * chunk, (g % grouped + 1) * chunk)
            if g % grouped == 0:
                for copy in part_copies[lot][cut]:
                    copy.wait_recv()
            if g == 0:
                total = part[lot, 0, c, :, width:]
                for k in range(1, cols):
                    total = total + part_in[lot, 0, k - 1, :, width:]
                factor = lax.rsqrt(total / D + 1e-05)
            total = part[lot, cut, c, :, lanes]
            for k in range(1, cols):
                total = total + part_in[lot, cut, k - 1, :, lanes]
            cut = [total[:, i * head_dim : (i + 1) * head_dim] * factor for i in range(per + 2)]
            new_key = rotate(cut[per]).astype(jnp.bfloat16).astype(jnp.float32)
            new_value = cut[per + 1].astype(jnp.bfloat16).astype(jnp.float32)
            for i in range(per):
                at = pl.ds((g * per + i) * own, own)
                q_rows[lot, at, :] = rotate(cut[i])
                k_rows[lot, at, :] = new_key
                v_rows[lot, at, :] = new_value
        taken = [pl.ds(i, heads, stride=own) for i in seqs]
        queries = [q_rows[lot, taken[i], :].astype(jnp.bfloat16) for i in seqs]
        scores = [
            lax.dot_general(
                queries[i],
                keys[lot * own + i],
                (((1,), (1,)), ((), ())),
                preferred_element_type=jnp.float32,
            )
            * scale
            for i in seqs
        ]
        own_scores = [
            jnp.sum(
                queries[i].astype(jnp.float32) * k_rows[lot, taken[i], :], axis=1, keepdims=True
            )
            * scale
            for i in seqs
        ]
        weights, own_weights = [], []
        for i in seqs:
            visible = same_group & (spot_at < length_of[lot][i] * groups)
            masked = jnp.where(visible, scores[i], -jnp.inf)
            row_max = jnp.maximum(jnp.max(masked, axis=1, keepdims=True), own_scores[i])
            cache_exp = jnp.exp(masked - row_max)
            own_exp = jnp.exp(own_scores[i] - row_max)
            total = jnp.sum(cache_exp, axis=1, keepdims=True) + own_exp
            weights.append((cache_exp / total).astype(jnp.bfloat16))
            own_weights.append((own_exp / total).astype(jnp.bfloat16).astype(jnp.float32))
        for i in seqs:
            result = jnp.dot(
                weights[i], values[lot * own + i], preferred_element_type=jnp.float32
            )
            a_rows[lot, taken[i], :] = result + own_weights[i] * v_rows[lot, taken[i], :]
        for h in range(heads):
            attended[lot, c, :, h * head_dim : (h + 1) * head_dim] = a_rows[
                lot, h * own : (h + 1) * own, :
            ].astype(jnp.bfloat16)
        started = []
        for k in range(1, cols):
            peer = lax.rem(c + k, cols)
            started.append(
                remote(
                    attended.at[lot, c],
                    attended.at[lot, c],
                    at_send.at[lot, k - 1],
                    at_recv.at[lot, k - 1],
                    (s, r, peer),
                )
            )
            started[-1].start()
        attended_copies.append(started)
        copies += started

    load_wo.wait()

    def onward(lot, n, other):
        return remote(
            mixed.at[lot, r, n],
            arrived.at[lot, r, n],
            x_send.at[lot, n, other],
            x_recv.at[lot, n, r],
            (lax.rem(s + 1, sections), other, c),
        )

    def sideways(lot, n, k):
        return remote(
            mixed.at[lot, r, n],
            mixed.at[lot, r, n],
            y_send.at[lot, n, k - 1],
            y_recv.at[lot, n, k - 1],
            (s, lax.rem(r + k, row_count), c),
        )

    for lot in range(lots):
        for copy in attended_copies[lot]:
            copy.wait_recv()
        for at in range(cols):
            gathered[lot, at * own : (at + 1) * own, :] = attended[lot, at].astype(jnp.float32)
        everyone = gathered[lot].astype(jnp.bfloat16)
        for n in range(pieces):
            at = slice(n * piece, (n + 1) * piece)
            product = jnp.dot(everyone, wo[:, at], preferred_element_type=jnp.float32)
            mixed[lot, r, n] = product + jnp.where(r == 0, state[lot, :, at], 0.0)

            @pl.when(s < sections - 1)
            def _():
                for other in range(row_count):
                    onward(lot, n, other).start()

            @pl.when(s == sections - 1)
            def _():
                for k in range(1, row_count):
                    sideways(lot, n, k).start()

    @pl.when(s < sections - 1)
    def _():
        for lot in range(lots):
            for n in range(pieces):
                for k in range(1, row_count):
                    sideways(lot, n, k).start()

    for lot in range(lots):
        for n in range(pieces):
            for k in range(1, row_count):
                sideways(lot, n, k).wait_recv()
            total = mixed[lot, 0, n]
            for other in range(1, row_count):
                total = total + mixed[lot, other, n]
            final = jnp.dot(back, total.astype(jnp.bfloat16), preferred_element_type=jnp.float32)
            out[lot * micro : (lot + 1) * micro, :, n * piece : (n + 1) * piece] = final.reshape(
                micro, batch, piece
            ).astype(jnp.bfloat16)

    for copy in copies:
        copy.wait_send()
    for lot in range(lots):
        for n in range(pieces):
            for k in range(1, row_count):
                sideways(lot, n, k).wait_send()

    @pl.when(s < sections - 1)
    def _():
        for lot in range(lots):
            for n in range(pieces):
                for other in range(row_count):
                    onward(lot, n, other).wait_send()


def shards(hidden, norm_gain, w_qkv, w_out, cache_keys, cache_values, cache_lengths):
    sections, row_count, cols = (lax.axis_size(a) for a in ("section", "row", "col"))
    micro, batch, depth = hidden.shape
    rows = micro // LOTS * batch
    own = rows // cols
    spots, groups, head_dim = cache_keys.shape[3:]
    per = HEADS // KVH
    heads = groups * per
    chunk = (per + 2) * head_dim
    piece = min(PIECE, w_out.shape[2])
    cuts = min(CUTS, groups)
    width = groups // cuts * chunk + head_dim
    pieces = w_out.shape[2] // piece
    keys = cache_keys.reshape(LOTS * own, spots * groups, head_dim)
    values = cache_values.reshape(LOTS * own, spots * groups, head_dim)
    vmem = pl.BlockSpec(memory_space=pltpu.VMEM)
    hbm = pl.BlockSpec(memory_space=pl.ANY)
    dma = pltpu.SemaphoreType.DMA
    f32, bf16 = jnp.float32, jnp.bfloat16
    return pl.pallas_call(
        functools.partial(kernel, (sections, row_count, cols)),
        out_shape=pltpu.VMEM((micro, batch, depth), bf16),
        in_specs=[hbm] * 7,
        out_specs=vmem,
        scratch_shapes=[
            pltpu.VMEM(hidden.shape, bf16),
            pltpu.VMEM(norm_gain.shape, bf16),
            pltpu.SMEM(cache_lengths.T.shape, jnp.int32),
            pltpu.VMEM((groups, depth, chunk), bf16),
            pltpu.VMEM(w_out.shape[1:], bf16),
            pltpu.VMEM(keys.shape, bf16),
            pltpu.VMEM(values.shape, bf16),
            pltpu.VMEM((LOTS, rows, depth), f32),
            pltpu.VMEM((LOTS, cuts, cols, own, width), f32),
            pltpu.VMEM((LOTS, cuts, cols - 1, own, width), f32),
            pltpu.VMEM((LOTS, heads * own, head_dim), f32),
            pltpu.VMEM((LOTS, heads * own, head_dim), f32),
            pltpu.VMEM((LOTS, heads * own, head_dim), f32),
            pltpu.VMEM((LOTS, heads * own, head_dim), f32),
            pltpu.VMEM((LOTS, cols, own, heads * head_dim), bf16),
            pltpu.VMEM((LOTS, rows, heads * head_dim), f32),
            pltpu.VMEM((LOTS, row_count, pieces, rows, piece), f32),
            pltpu.VMEM((LOTS, row_count, pieces, rows, piece), f32),
            dma((groups + 6,)),
            dma((LOTS, cuts, cols - 1)),
            dma((LOTS, cuts, cols - 1)),
            dma((LOTS, cols - 1)),
            dma((LOTS, cols - 1)),
            dma((LOTS, pieces, row_count)),
            dma((LOTS, pieces, row_count)),
            dma((LOTS, pieces, row_count - 1)),
            dma((LOTS, pieces, row_count - 1)),
        ],
        compiler_params=pltpu.CompilerParams(collective_id=0, has_side_effects=True),
    )(hidden, norm_gain, w_qkv[0], w_out[0], keys, values, cache_lengths.T)[None]


def solution(mesh):
    return jax.shard_map(
        shards,
        mesh=mesh,
        in_specs=(
            P(None, None, "col"),
            P("section", "col"),
            P("section", "col", "row"),
            P("section", "row", "col"),
            P("section", None, "col", None, "row", None),
            P("section", None, "col", None, "row", None),
            P(None, "col"),
        ),
        out_specs=P("section", None, None, "col"),
        check_vma=False,
    )
```

```python
import functools
import math

import jax
import jax.numpy as jnp
from jax import lax
from jax.experimental import pallas as pl
from jax.experimental.pallas import tpu as pltpu
from jax.sharding import PartitionSpec as P

D = 4096
HEADS = 32
KVH = 8
LOTS = 4
CUTS = 2
PIECE = 1024
MESH = pl.DeviceIdType.MESH


def remainder(values, by):
    if by & (by - 1) == 0:
        return values & (by - 1)
    return lax.rem(values, jnp.full_like(values, by))


def kernel(
    dims,
    hidden_hbm,
    gain_hbm,
    wq_hbm,
    wo_hbm,
    keys_hbm,
    values_hbm,
    lengths_hbm,
    out,
    hidden,
    gain,
    lengths,
    wq,
    wo,
    keys,
    values,
    state,
    part,
    part_in,
    q_rows,
    k_rows,
    v_rows,
    a_rows,
    attended,
    gathered,
    mixed,
    arrived,
    load_sem,
    rs_send,
    rs_recv,
    at_send,
    at_recv,
    x_send,
    x_recv,
    y_send,
    y_recv,
):
    sections, row_count, cols = dims
    s = lax.axis_index("section")
    r = lax.axis_index("row")
    c = lax.axis_index("col")
    batch, depth = hidden.shape[1:]
    lots, rows = state.shape[:2]
    micro = rows // batch
    own = rows // cols
    seq_part = batch // cols
    groups, chunk = wq.shape[0], wq.shape[2]
    head_dim = keys.shape[2]
    per = HEADS // KVH
    heads = groups * per
    spots = keys.shape[1]
    pieces, piece = mixed.shape[2], mixed.shape[4]
    cuts = part.shape[1]
    grouped = groups // cuts
    width = grouped * chunk

    def remote(src, dst, send_sem, recv_sem, device):
        return pltpu.make_async_remote_copy(
            src_ref=src,
            dst_ref=dst,
            send_sem=send_sem,
            recv_sem=recv_sem,
            device_id=device,
            device_id_type=MESH,
        )

    loads = [
        pltpu.make_async_copy(
            wq_hbm.at[:, pl.ds(g * chunk, chunk)], wq.at[g], load_sem.at[g]
        )
        for g in range(groups)
    ]
    load_keys = pltpu.make_async_copy(keys_hbm, keys, load_sem.at[groups])
    load_values = pltpu.make_async_copy(values_hbm, values, load_sem.at[groups + 1])
    load_wo = pltpu.make_async_copy(wo_hbm, wo, load_sem.at[groups + 2])
    load_lengths = pltpu.make_async_copy(lengths_hbm, lengths, load_sem.at[groups + 3])
    load_hidden = pltpu.make_async_copy(hidden_hbm, hidden, load_sem.at[groups + 4])
    load_gain = pltpu.make_async_copy(gain_hbm, gain, load_sem.at[groups + 5])
    for load in [load_lengths, load_hidden, load_gain] + loads + [load_keys, load_values, load_wo]:
        load.start()

    if cols % 2 == 0:
        peers = [
            lax.rem(k - c + cols, cols) if k % 2 else lax.rem(c + k, cols)
            for k in range(cols - 1, 0, -1)
        ]
    else:
        peers = [lax.rem(c + k, cols) for k in range(1, cols)]

    barrier = pltpu.get_barrier_semaphore()
    greeted = 0
    for k in range(1, cols):
        pl.semaphore_signal(
            barrier, inc=1, device_id=(s, r, peers[k - 1]), device_id_type=MESH
        )
        greeted += 1
    for k in range(1, row_count):
        pl.semaphore_signal(
            barrier, inc=1, device_id=(s, lax.rem(r + k, row_count), c), device_id_type=MESH
        )
        greeted += 1
    for step in (1, sections - 1):
        for other in range(row_count):
            pl.semaphore_signal(
                barrier,
                inc=1,
                device_id=(lax.rem(s + step, sections), other, c),
                device_id_type=MESH,
            )
            greeted += 1

    to_row = lax.broadcasted_iota(jnp.int32, (rows, rows), 0)
    from_row = lax.broadcasted_iota(jnp.int32, (rows, rows), 1)
    order = jnp.zeros((rows, rows), jnp.bool_)
    back = jnp.zeros((rows, rows), jnp.bool_)
    for at in range(cols):
        for m in range(micro):
            first, source = at * own + m * seq_part, m * batch + at * seq_part
            inside = (to_row >= first) & (to_row < first + seq_part)
            order = order | (inside & (to_row - from_row == first - source))
            inside = (from_row >= first) & (from_row < first + seq_part)
            back = back | (inside & (from_row - to_row == first - source))
    order = jnp.where(order, 1.0, 0.0).astype(jnp.bfloat16)
    back = jnp.where(back, 1.0, 0.0).astype(jnp.bfloat16)

    row_at = lax.broadcasted_iota(jnp.int32, (own, head_dim), 0)
    lane = lax.broadcasted_iota(jnp.int32, (own, head_dim), 1)
    half = head_dim // 2
    half_lane = jnp.where(lane < half, lane, lane - half).astype(jnp.float32)
    frequency = jnp.exp(half_lane * (-2.0 * math.log(500000.0) / head_dim))
    load_lengths.wait()
    length_of, cosines, sines = [], [], []
    for lot in range(lots):
        position = jnp.zeros((own, head_dim), jnp.float32)
        length_of.append([])
        for i in range(own):
            length = lengths[i % seq_part, lot * micro + i // seq_part]
            length_of[lot].append(length)
            position = jnp.where(row_at == i, length.astype(jnp.float32), position)
        angles = position * frequency
        cosines.append(jnp.cos(angles))
        sine = jnp.sin(angles)
        sines.append(jnp.where(lane < half, -sine, sine))

    head_at = lax.broadcasted_iota(jnp.int32, (heads, spots), 0)
    spot_at = lax.broadcasted_iota(jnp.int32, (heads, spots), 1)
    head_group = jnp.zeros((heads, spots), jnp.int32)
    for g in range(1, groups):
        head_group = head_group + jnp.where(head_at >= g * per, 1, 0)
    same_group = remainder(spot_at, groups) == head_group

    load_hidden.wait()
    load_gain.wait()

    @pl.when(s == 0)
    def _():
        for lot in range(lots):
            entry = hidden[lot * micro : (lot + 1) * micro].astype(jnp.float32)
            entry = entry.reshape(rows, depth).astype(jnp.bfloat16)
            state[lot] = jnp.dot(order, entry, preferred_element_type=jnp.float32)

    pl.semaphore_wait(barrier, greeted)

    copies = []
    part_copies, attended_copies = [], []
    for lot in range(lots):
        @pl.when(s > 0)
        def _():
            for n in range(pieces):
                for other in range(row_count):
                    remote(
                        mixed.at[lot, 0, n],
                        arrived.at[lot, other, n],
                        x_send.at[lot, n, 0],
                        x_recv.at[lot, n, other],
                        (s, r, c),
                    ).wait_recv()
                total = arrived[lot, 0, n]
                for other in range(1, row_count):
                    total = total + arrived[lot, other, n]
                state[lot, :, n * piece : (n + 1) * piece] = total.astype(jnp.bfloat16).astype(
                    jnp.float32
                )

        current = state[lot]
        squares = jnp.sum(current * current, axis=1, keepdims=True)
        squares = jnp.broadcast_to(squares, (rows, head_dim))
        for at in range(cols):
            part[lot, 0, at, :, width:] = squares[at * own : (at + 1) * own]
        scaled = (current * gain[...].astype(jnp.float32)).astype(jnp.bfloat16)
        part_copies.append([])
        for g in range(groups):
            if lot == 0:
                loads[g].wait()
            product = jnp.dot(scaled, wq[g], preferred_element_type=jnp.float32)
            cut, at_lane = g // grouped, g % grouped * chunk
            for at in range(cols):
                part[lot, cut, at, :, at_lane : at_lane + chunk] = product[
                    at * own : (at + 1) * own
                ]
            if (g + 1) % grouped:
                continue
            started = []
            sent = pl.ds(0, width + head_dim if cut == 0 else width)
            for k in range(1, cols):
                peer = peers[k - 1]
                started.append(
                    remote(
                        part.at[lot, cut, peer, :, sent],
                        part_in.at[lot, cut, k - 1, :, sent],
                        rs_send.at[lot, cut, k - 1],
                        rs_recv.at[lot, cut, k - 1],
                        (s, r, peer),
                    )
                )
                started[-1].start()
            part_copies[lot].append(started)
            copies += started

    load_keys.wait()
    load_values.wait()
    scale = 1.0 / math.sqrt(head_dim)
    seqs = range(own)
    for lot in range(lots):

        def rotate(vectors):
            return vectors * cosines[lot] + pltpu.roll(vectors, half, 1) * sines[lot]

        for g in range(groups):
            cut, lanes = g // grouped, slice(g % grouped * chunk, (g % grouped + 1) * chunk)
            if g % grouped == 0:
                for copy in part_copies[lot][cut]:
                    copy.wait_recv()
            if g == 0:
                total = part[lot, 0, c, :, width:]
                for k in range(1, cols):
                    total = total + part_in[lot, 0, k - 1, :, width:]
                factor = lax.rsqrt(total / D + 1e-05)
            total = part[lot, cut, c, :, lanes]
            for k in range(1, cols):
                total = total + part_in[lot, cut, k - 1, :, lanes]
            cut = [total[:, i * head_dim : (i + 1) * head_dim] * factor for i in range(per + 2)]
            new_key = rotate(cut[per]).astype(jnp.bfloat16).astype(jnp.float32)
            new_value = cut[per + 1].astype(jnp.bfloat16).astype(jnp.float32)
            for i in range(per):
                at = pl.ds((g * per + i) * own, own)
                q_rows[lot, at, :] = rotate(cut[i])
                k_rows[lot, at, :] = new_key
                v_rows[lot, at, :] = new_value
        taken = [pl.ds(i, heads, stride=own) for i in seqs]
        queries = [q_rows[lot, taken[i], :].astype(jnp.bfloat16) for i in seqs]
        scores = [
            lax.dot_general(
                queries[i],
                keys[lot * own + i],
                (((1,), (1,)), ((), ())),
                preferred_element_type=jnp.float32,
            )
            * scale
            for i in seqs
        ]
        own_scores = [
            jnp.sum(
                queries[i].astype(jnp.float32) * k_rows[lot, taken[i], :], axis=1, keepdims=True
            )
            * scale
            for i in seqs
        ]
        weights, own_weights = [], []
        for i in seqs:
            visible = same_group & (spot_at < length_of[lot][i] * groups)
            masked = jnp.where(visible, scores[i], -jnp.inf)
            row_max = jnp.maximum(jnp.max(masked, axis=1, keepdims=True), own_scores[i])
            cache_exp = jnp.exp(masked - row_max)
            own_exp = jnp.exp(own_scores[i] - row_max)
            total = jnp.sum(cache_exp, axis=1, keepdims=True) + own_exp
            weights.append((cache_exp / total).astype(jnp.bfloat16))
            own_weights.append((own_exp / total).astype(jnp.bfloat16).astype(jnp.float32))
        for i in seqs:
            result = jnp.dot(
                weights[i], values[lot * own + i], preferred_element_type=jnp.float32
            )
            a_rows[lot, taken[i], :] = result + own_weights[i] * v_rows[lot, taken[i], :]
        for h in range(heads):
            attended[lot, c, :, h * head_dim : (h + 1) * head_dim] = a_rows[
                lot, h * own : (h + 1) * own, :
            ].astype(jnp.bfloat16)
        started = []
        for k in range(1, cols):
            peer = peers[k - 1]
            started.append(
                remote(
                    attended.at[lot, c],
                    attended.at[lot, c],
                    at_send.at[lot, k - 1],
                    at_recv.at[lot, k - 1],
                    (s, r, peer),
                )
            )
            started[-1].start()
        attended_copies.append(started)
        copies += started

    load_wo.wait()

    def onward(lot, n, other):
        return remote(
            mixed.at[lot, r, n],
            arrived.at[lot, r, n],
            x_send.at[lot, n, other],
            x_recv.at[lot, n, r],
            (lax.rem(s + 1, sections), lax.rem(r + 1 + other, row_count), c),
        )

    def sideways(lot, n, k):
        return remote(
            mixed.at[lot, r, n],
            mixed.at[lot, r, n],
            y_send.at[lot, n, k - 1],
            y_recv.at[lot, n, k - 1],
            (s, lax.rem(r + k, row_count), c),
        )

    for lot in range(lots):
        for copy in attended_copies[lot]:
            copy.wait_recv()
        for at in range(cols):
            gathered[lot, at * own : (at + 1) * own, :] = attended[lot, at].astype(jnp.float32)
        everyone = gathered[lot].astype(jnp.bfloat16)
        for n in range(pieces):
            at = slice(n * piece, (n + 1) * piece)
            product = jnp.dot(everyone, wo[:, at], preferred_element_type=jnp.float32)
            mixed[lot, r, n] = product + jnp.where(r == 0, state[lot, :, at], 0.0)

            @pl.when(s < sections - 1)
            def _():
                for other in range(row_count):
                    onward(lot, n, other).start()

            @pl.when(s == sections - 1)
            def _():
                for k in range(1, row_count):
                    sideways(lot, n, k).start()

    @pl.when(s < sections - 1)
    def _():
        for lot in range(lots):
            for n in range(pieces):
                for k in range(1, row_count):
                    sideways(lot, n, k).start()

    for lot in range(lots):
        for n in range(pieces):
            for k in range(1, row_count):
                sideways(lot, n, k).wait_recv()
            total = mixed[lot, 0, n]
            for other in range(1, row_count):
                total = total + mixed[lot, other, n]
            final = jnp.dot(back, total.astype(jnp.bfloat16), preferred_element_type=jnp.float32)
            out[lot * micro : (lot + 1) * micro, :, n * piece : (n + 1) * piece] = final.reshape(
                micro, batch, piece
            ).astype(jnp.bfloat16)

    for copy in copies:
        copy.wait_send()
    for lot in range(lots):
        for n in range(pieces):
            for k in range(1, row_count):
                sideways(lot, n, k).wait_send()

    @pl.when(s < sections - 1)
    def _():
        for lot in range(lots):
            for n in range(pieces):
                for other in range(row_count):
                    onward(lot, n, other).wait_send()


def shards(hidden, norm_gain, w_qkv, w_out, cache_keys, cache_values, cache_lengths):
    sections, row_count, cols = (lax.axis_size(a) for a in ("section", "row", "col"))
    micro, batch, depth = hidden.shape
    rows = micro // LOTS * batch
    own = rows // cols
    spots, groups, head_dim = cache_keys.shape[3:]
    per = HEADS // KVH
    heads = groups * per
    chunk = (per + 2) * head_dim
    piece = min(PIECE, w_out.shape[2])
    cuts = min(CUTS, groups)
    width = groups // cuts * chunk + head_dim
    pieces = w_out.shape[2] // piece
    keys = cache_keys.reshape(LOTS * own, spots * groups, head_dim)
    values = cache_values.reshape(LOTS * own, spots * groups, head_dim)
    vmem = pl.BlockSpec(memory_space=pltpu.VMEM)
    hbm = pl.BlockSpec(memory_space=pl.ANY)
    dma = pltpu.SemaphoreType.DMA
    f32, bf16 = jnp.float32, jnp.bfloat16
    return pl.pallas_call(
        functools.partial(kernel, (sections, row_count, cols)),
        out_shape=pltpu.VMEM((micro, batch, depth), bf16),
        in_specs=[hbm] * 7,
        out_specs=vmem,
        scratch_shapes=[
            pltpu.VMEM(hidden.shape, bf16),
            pltpu.VMEM(norm_gain.shape, bf16),
            pltpu.SMEM(cache_lengths.T.shape, jnp.int32),
            pltpu.VMEM((groups, depth, chunk), bf16),
            pltpu.VMEM(w_out.shape[1:], bf16),
            pltpu.VMEM(keys.shape, bf16),
            pltpu.VMEM(values.shape, bf16),
            pltpu.VMEM((LOTS, rows, depth), f32),
            pltpu.VMEM((LOTS, cuts, cols, own, width), f32),
            pltpu.VMEM((LOTS, cuts, cols - 1, own, width), f32),
            pltpu.VMEM((LOTS, heads * own, head_dim), f32),
            pltpu.VMEM((LOTS, heads * own, head_dim), f32),
            pltpu.VMEM((LOTS, heads * own, head_dim), f32),
            pltpu.VMEM((LOTS, heads * own, head_dim), f32),
            pltpu.VMEM((LOTS, cols, own, heads * head_dim), bf16),
            pltpu.VMEM((LOTS, rows, heads * head_dim), f32),
            pltpu.VMEM((LOTS, row_count, pieces, rows, piece), f32),
            pltpu.VMEM((LOTS, row_count, pieces, rows, piece), f32),
            dma((groups + 6,)),
            dma((LOTS, cuts, cols - 1)),
            dma((LOTS, cuts, cols - 1)),
            dma((LOTS, cols - 1)),
            dma((LOTS, cols - 1)),
            dma((LOTS, pieces, row_count)),
            dma((LOTS, pieces, row_count)),
            dma((LOTS, pieces, row_count - 1)),
            dma((LOTS, pieces, row_count - 1)),
        ],
        compiler_params=pltpu.CompilerParams(collective_id=0, has_side_effects=True),
    )(hidden, norm_gain, w_qkv[0], w_out[0], keys, values, cache_lengths.T)[None]


def solution(mesh):
    return jax.shard_map(
        shards,
        mesh=mesh,
        in_specs=(
            P(None, None, "col"),
            P("section", "col"),
            P("section", "col", "row"),
            P("section", "row", "col"),
            P("section", None, "col", None, "row", None),
            P("section", None, "col", None, "row", None),
            P(None, "col"),
        ),
        out_specs=P("section", None, None, "col"),
        check_vma=False,
    )
```
